32 devices in a mesh: row: 8 (over y, x, core), col: 4 (over z).
Axes of the slice: x: 2, y: 2, z: 4, core: 2. Of those that a mesh axis runs over, the one named last changes fastest.
Arguments:
- record: float32 [2, 32768], P(None, ('row', 'col')), may hold values from -5 to 5
Outputs:
- spectrum: float32 [256, 256, 2, 2, 256], P('row', 'col')
The draws below stay inside these ranges and needn't reach their ends.
All inputs are finite; a program needn't handle non-finite values.
Results may differ from the reference program's by a relative error of at most 0.00011.
Values sent between devices are 32-bit elements; how exact they have to be, the bound alone decides.
No kernel may reach another device: no remote copies, remote signals or barrier semaphores. Data moves between devices by JAX's collectives and lax.ppermute only.
A program may use at most 64 MiB of HBM per device.

```python
import math
import jax
import jax.numpy as jnp
from jax import lax

C = 256
P_SIZE = 256
HOP = 64
FRAMES = 512
SAMPLES = 32768


def block_scale(own_key, shape, shards, least, high):
    loudness = 1.0
    for dim, blocks in shards:
        draws = jax.random.uniform(jax.random.fold_in(jax.random.fold_in(own_key, 6), dim), (blocks,), jnp.float32, least / len(shards), high / len(shards))
        loudness = loudness * jnp.repeat(jnp.exp(draws), shape[dim] // blocks).reshape((-1,) + (1,) * (len(shape) - 1 - dim))
    return loudness


def scatter_about(stream_key, shape, spread, bound, pieces=(), held_as=jnp.bfloat16):
    level = block_scale(stream_key, shape, pieces, -0.22, 0.18) if pieces else 1.0
    values = jax.random.normal(stream_key, shape, jnp.float32) * spread * level
    return jnp.minimum(jnp.maximum(values, -bound), bound).astype(held_as)


def setup_inputs(seed: int = 0) -> dict:
    splits = jax.random.split(jax.random.key(seed), 2)
    return {
        "record": scatter_about(splits[0], (2, SAMPLES), 0.7, 5.0, ((1, 32),), jnp.float32),
    }


highest = lax.Precision.HIGHEST

def spectral_table(length, start_column, width, weights):
    position = jnp.arange(length, dtype=jnp.int32)
    column = start_column + jnp.arange(width, dtype=jnp.int32)
    turns = position[:, None] * column[None, :] % length
    phase = turns.astype(jnp.float32) * (2.0 * math.pi / length)
    cosine = weights[:, None] * jnp.cos(phase)
    sinus = weights[:, None] * jnp.sin(phase)
    upper = jnp.stack([cosine, -sinus], axis=1)
    bottom = jnp.stack([sinus, cosine], axis=1)
    return jnp.stack([upper, bottom], axis=0)

def hann_weights():
    position = jnp.arange(C, dtype=jnp.int32).astype(jnp.float32)
    return (0.5 - 0.5 * jnp.cos(position * (2.0 * math.pi / C))) / math.sqrt(3.0 * C / 8.0)

def framed(samples, amount):
    blocks = samples.reshape(2, amount + C // HOP - 1, HOP)
    return jnp.concatenate([blocks[:, offset:offset + amount] for offset in range(C // HOP)], axis=2)

def downconvert(spectra, start_channel, start_frame):
    channel = start_channel + jnp.arange(spectra.shape[1], dtype=jnp.int32)
    moment = start_frame + jnp.arange(spectra.shape[2], dtype=jnp.int32)
    turns = (channel * HOP % C)[:, None] * (moment % C)[None, :] % C
    phase = turns.astype(jnp.float32) * (2.0 * math.pi / C)
    cosine = jnp.cos(phase)
    sinus = jnp.sin(phase)
    real_part = spectra[0] * cosine + spectra[1] * sinus
    imag_part = spectra[1] * cosine - spectra[0] * sinus
    return jnp.stack([real_part, imag_part])

def channelize(frames, start_channel, width, start_frame):
    weights = spectral_table(C, start_channel, width, hann_weights())
    spectra = lax.dot_general(weights, frames, (((0, 1), (0, 2)), ((), ())), precision=highest, preferred_element_type=jnp.float32)
    return downconvert(spectra, start_channel, start_frame)

def correlate(leading, trailing):
    lead_count = leading.shape[1]
    trail_count = trailing.shape[1]
    windows = leading.shape[2] // P_SIZE
    lead = leading.reshape(2, lead_count, windows, P_SIZE)
    trail = trailing.reshape(2, trail_count, windows, P_SIZE)
    real_part = lead[0][:, None] * trail[0][None] + lead[1][:, None] * trail[1][None]
    imag_part = lead[1][:, None] * trail[0][None] - lead[0][:, None] * trail[1][None]
    weights = spectral_table(P_SIZE, 0, P_SIZE, jnp.full((P_SIZE,), 1.0 / math.sqrt(P_SIZE), jnp.float32))
    real_table = weights[0].reshape(P_SIZE, 2 * P_SIZE)
    imag_table = weights[1].reshape(P_SIZE, 2 * P_SIZE)
    dims = (((3,), (0,)), ((), ()))
    result = lax.dot_general(real_part, real_table, dims, precision=highest, preferred_element_type=jnp.float32)
    result = result + lax.dot_general(imag_part, imag_table, dims, precision=highest, preferred_element_type=jnp.float32)
    return result.reshape(lead_count, trail_count, windows, 2, P_SIZE)

def reference(record):
    samples = jnp.concatenate([record, jnp.zeros((2, C - HOP), jnp.float32)], axis=1)
    frames = framed(samples, FRAMES)
    spectra = channelize(frames, 0, C, 0)

    def one_channel(which):
        leading = lax.dynamic_slice_in_dim(spectra, which, 1, 1)
        return correlate(leading, spectra)[0]
    return lax.map(one_channel, jnp.arange(C, dtype=jnp.int32))
```

```python
import functools
import math

import jax
import jax.numpy as jnp
import numpy as np
from jax import lax
from jax.experimental import pallas as pl
from jax.experimental.pallas import tpu as pltpu
from jax.sharding import PartitionSpec as P

C = 256
P_SIZE = 256
HOP = 64
LANES = 128
HALF = P_SIZE // 2
GROUP = 4


def split_table(table):
    high = table.astype(jnp.bfloat16)
    low = (table - high.astype(np.float64)).astype(jnp.bfloat16)
    return high, low


def channel_table():
    m = np.arange(C)
    hann = (0.5 - 0.5 * np.cos(2.0 * math.pi * m / C)) / math.sqrt(3.0 * C / 8.0)
    phase = 2.0 * math.pi * (np.arange(C)[:, None] * m[None, :] % C) / C
    cosine = hann * np.cos(phase)
    sinus = hann * np.sin(phase)
    upper = np.concatenate([cosine, sinus], axis=1)
    lower = np.concatenate([-sinus, cosine], axis=1)
    return np.stack([upper, lower])


def window_table(odd):
    p = 2 * np.arange(HALF) + odd
    phase = 2.0 * math.pi * (p[:, None] * np.arange(HALF)[None, :] % P_SIZE) / P_SIZE
    cosine = np.cos(phase) / math.sqrt(P_SIZE)
    sinus = np.sin(phase) / math.sqrt(P_SIZE)
    upper = np.concatenate([cosine, -sinus], axis=1)
    lower = np.concatenate([sinus, cosine], axis=1)
    return np.concatenate([upper, lower], axis=0)


def halves(x):
    high = x.astype(jnp.bfloat16)
    return high, (x - high.astype(jnp.float32)).astype(jnp.bfloat16)


def dot(a, b, contract=(1, 0)):
    return lax.dot_general(
        a,
        b,
        (((contract[0],), (contract[1],)), ((), ())),
        preferred_element_type=jnp.float32,
    )


def slot_of(index, order):
    return sum(((index >> bit) & 1) << stage for stage, bit in enumerate(order))


def kernel(order, sizes, key_ref, rec_ref, lead_ref, trail_ref, dft_ref, out_ref,
           real_ref, imag_ref, frame_ref, first_ref, second_ref, z_ref):
    devices, lead_width, trail_width, windows = sizes
    rows = devices * rec_ref.shape[1] // 2
    block = rec_ref.shape[1] // 2
    pattern = first_ref.shape[2]

    @pl.when(pl.program_id(0) == 0)
    def _():
        key = key_ref[0]
        for device in range(devices):
            slot = key ^ slot_of(device, order)
            piece = rec_ref[slot]
            real_ref[device * block : (device + 1) * block] = piece[:block]
            imag_ref[device * block : (device + 1) * block] = piece[block:]
        zeros = jnp.zeros((8, LANES), jnp.float32)
        real_ref[rows : rows + 8] = zeros
        imag_ref[rows : rows + 8] = zeros
        lower = lax.broadcasted_iota(jnp.int32, (HALF, LANES), 1) < HOP
        table = [jnp.concatenate([lead_ref[i, 0], lead_ref[i, 1], trail_ref[i, 0], trail_ref[i, 1]])
                 for i in range(2)]
        for window in range(windows):
            for part, ref in enumerate((real_ref, imag_ref)):
                shifts = [ref[window * HALF + i : window * HALF + i + HALF] for i in range(3)]
                turned = [pltpu.roll(x, HOP, 1) for x in shifts]
                odd = [jnp.where(lower, turned[i], turned[i + 1]) for i in range(2)]
                for start, pieces in ((0, shifts[:2]), (HALF, odd)):
                    for i, piece in enumerate(pieces):
                        high, low = halves(piece)
                        column = (2 * part + i) * LANES
                        frame_ref[0, start : start + HALF, column : column + LANES] = high
                        frame_ref[1, start : start + HALF, column : column + LANES] = low
            spectra = dot(table[0], frame_ref[0], (1, 1))
            spectra += dot(table[0], frame_ref[1], (1, 1))
            spectra += dot(table[1], frame_ref[0], (1, 1))
            start = 0
            for which, width in enumerate((lead_width, trail_width)):
                real = spectra[start : start + width]
                imag = spectra[start + width : start + 2 * width]
                start += 2 * width
                channel = lax.broadcasted_iota(jnp.int32, (width, HALF), 0)
                frame = lax.broadcasted_iota(jnp.int32, (width, HALF), 1)
                sign = jnp.where(channel & frame & 1 == 1, -1.0, 1.0)
                is_odd = channel & 1 == 1
                real_sign = jnp.where(channel & 3 >= 2, -sign, sign)
                imag_sign = jnp.where((channel + 1) & 3 >= 2, -sign, sign)
                values = (
                    real[:, :HALF] * sign,
                    imag[:, :HALF] * sign,
                    jnp.where(is_odd, imag[:, HALF:], real[:, HALF:]) * real_sign,
                    jnp.where(is_odd, real[:, HALF:], imag[:, HALF:]) * imag_sign,
                )
                for i, value in enumerate(values):
                    if which:
                        second_ref[i, pl.ds(window, width, stride=windows), :] = value
                    else:
                        for copy in range(pattern // windows):
                            first_ref[i, :, copy * windows + window, :] = value

    step = pl.program_id(0)
    height = trail_width * windows
    for local in range(GROUP):
        which = step * GROUP + local
        for start in range(0, height, pattern):
            lead = [first_ref[i, which] for i in range(4)]
            trail = [second_ref[i, start : start + pattern] for i in range(4)]
            for odd in range(2):
                ar, ai = lead[2 * odd : 2 * odd + 2]
                br, bi = trail[2 * odd : 2 * odd + 2]
                for part, value in enumerate((ar * br + ai * bi, ai * br - ar * bi)):
                    high, low = halves(value)
                    row = local * height + start
                    column = part * LANES
                    z_ref[odd, 0, row : row + pattern, column : column + LANES] = high
                    z_ref[odd, 1, row : row + pattern, column : column + LANES] = low
    chunk = min(256, height * GROUP)
    for row in range(0, height * GROUP, chunk):
        sums = []
        for odd in range(2):
            high = z_ref[odd, 0, row : row + chunk]
            low = z_ref[odd, 1, row : row + chunk]
            total = dot(high, dft_ref[odd, 0])
            total += dot(low, dft_ref[odd, 0])
            total += dot(high, dft_ref[odd, 1])
            sums.append(total)
        for i, value in enumerate((sums[0] + sums[1], sums[0] - sums[1])):
            for part in range(2):
                out_ref[pl.ds(row * 4 + 2 * i + part, chunk, stride=4), :] = value[
                    :, part * HALF : (part + 1) * HALF
                ]


def local(record):
    row_count = lax.axis_size("row")
    col_count = lax.axis_size("col")
    devices = row_count * col_count
    axes = ("row", "col")
    lead_width = C // row_count
    trail_width = C // col_count
    samples = record.shape[1]
    windows = samples * devices // HOP // P_SIZE
    row_index = lax.axis_index("row")
    col_index = lax.axis_index("col")
    me = row_index * col_count + col_index

    col_bits = list(range(col_count.bit_length() - 1))
    row_bits = list(range(len(col_bits), devices.bit_length() - 1))
    order = tuple(col_bits[::-1] + row_bits[1:] + row_bits[:1])
    blocks = record.reshape(1, 2 * samples // LANES, LANES)
    for bit in order:
        route = [(i, i ^ (1 << bit)) for i in range(devices)]
        blocks = jnp.concatenate([blocks, lax.ppermute(blocks, axes, route)], axis=0)

    table = jnp.asarray(np.stack(split_table(channel_table())))
    lead_table = lax.dynamic_slice_in_dim(table, row_index * lead_width, lead_width, 2)
    trail_table = lax.dynamic_slice_in_dim(table, col_index * trail_width, trail_width, 2)
    dft = jnp.asarray(np.stack([np.stack(split_table(window_table(odd))) for odd in range(2)]))
    key = slot_of(me, order).astype(jnp.int32).reshape(1)

    height = trail_width * windows
    pattern = max(8, windows)
    sizes = (devices, lead_width, trail_width, windows)
    vmem = pl.BlockSpec(memory_space=pltpu.VMEM)
    out = pl.pallas_call(
        functools.partial(kernel, order, sizes),
        grid=(lead_width // GROUP,),
        out_shape=jax.ShapeDtypeStruct((lead_width * height * 4, LANES), jnp.float32),
        in_specs=[pl.BlockSpec(memory_space=pltpu.SMEM), vmem, vmem, vmem, vmem],
        out_specs=pl.BlockSpec((GROUP * height * 4, LANES), lambda i: (i, 0)),
        scratch_shapes=[
            pltpu.VMEM((devices * samples // LANES + 8, LANES), jnp.float32),
            pltpu.VMEM((devices * samples // LANES + 8, LANES), jnp.float32),
            pltpu.VMEM((2, P_SIZE, 2 * C), jnp.bfloat16),
            pltpu.VMEM((4, lead_width, pattern, LANES), jnp.float32),
            pltpu.VMEM((4, height, LANES), jnp.float32),
            pltpu.VMEM((2, 2, GROUP * height, 2 * LANES), jnp.bfloat16),
        ],
        cost_estimate=pl.CostEstimate(flops=10**10, bytes_accessed=10**7, transcendentals=0),
    )(key, blocks, lead_table, trail_table, dft)
    out = out.reshape(lead_width, trail_width, windows, 2, 2, LANES)
    return out.transpose(0, 1, 2, 4, 3, 5).reshape(
        lead_width, trail_width, windows, 2, P_SIZE
    )


def solution(mesh):
    return jax.shard_map(
        local,
        mesh=mesh,
        in_specs=(P(None, ("row", "col")),),
        out_specs=P("row", "col", None, None, None),
        check_vma=False,
    )
```

```python
import functools
import math

import jax
import jax.numpy as jnp
import numpy as np
from jax import lax
from jax.experimental import pallas as pl
from jax.experimental.pallas import tpu as pltpu
from jax.sharding import PartitionSpec as P

C = 256
P_SIZE = 256
HOP = 64
LANES = 128
HALF = P_SIZE // 2
GROUP = 4


def split_table(table):
    high = table.astype(jnp.bfloat16)
    low = (table - high.astype(np.float64)).astype(jnp.bfloat16)
    return high, low


def channel_table():
    m = np.arange(C)
    hann = (0.5 - 0.5 * np.cos(2.0 * math.pi * m / C)) / math.sqrt(3.0 * C / 8.0)
    phase = 2.0 * math.pi * (np.arange(C)[:, None] * m[None, :] % C) / C
    cosine = hann * np.cos(phase)
    sinus = hann * np.sin(phase)
    upper = np.concatenate([cosine, sinus], axis=1)
    lower = np.concatenate([-sinus, cosine], axis=1)
    return np.stack([upper, lower])


def window_table(odd):
    p = 2 * np.arange(HALF) + odd
    phase = 2.0 * math.pi * (p[:, None] * np.arange(HALF)[None, :] % P_SIZE) / P_SIZE
    cosine = np.cos(phase) / math.sqrt(P_SIZE)
    sinus = np.sin(phase) / math.sqrt(P_SIZE)
    upper = np.concatenate([cosine, -sinus], axis=1)
    lower = np.concatenate([sinus, cosine], axis=1)
    return np.concatenate([upper, lower], axis=0)


def halves(x):
    high = x.astype(jnp.bfloat16)
    return high, (x - high.astype(jnp.float32)).astype(jnp.bfloat16)


def dot(a, b, contract=(1, 0)):
    return lax.dot_general(
        a,
        b,
        (((contract[0],), (contract[1],)), ((), ())),
        preferred_element_type=jnp.float32,
    )


def slot_of(index, order):
    return sum(((index >> bit) & 1) << stage for stage, bit in enumerate(order))


def fetch(widths, offset_ref, table_ref, dft_table_ref, weight_ref, dft_ref):
    start = 0
    for which, width in enumerate(widths):
        offset = pl.multiple_of(offset_ref[which], width)
        for part in range(2):
            for half in range(2):
                weight_ref[half, start : start + width] = table_ref[half, part, pl.ds(offset, width)]
            start += width
    dft_ref[...] = dft_table_ref[...]


def spectra_of(window, widths, real_ref, imag_ref, weight_ref, frame_ref):
    lower = lax.broadcasted_iota(jnp.int32, (HALF, LANES), 1) < HOP
    for part, ref in enumerate((real_ref, imag_ref)):
        shifts = [ref[window * HALF + i : window * HALF + i + HALF] for i in range(3)]
        turned = [pltpu.roll(x, HOP, 1) for x in shifts]
        odd = [jnp.where(lower, turned[i], turned[i + 1]) for i in range(2)]
        for start, pieces in ((0, shifts[:2]), (HALF, odd)):
            for i, piece in enumerate(pieces):
                high, low = halves(piece)
                column = (2 * part + i) * LANES
                frame_ref[0, start : start + HALF, column : column + LANES] = high
                frame_ref[1, start : start + HALF, column : column + LANES] = low
    spectra = dot(weight_ref[0], frame_ref[0], (1, 1))
    spectra += dot(weight_ref[0], frame_ref[1], (1, 1))
    spectra += dot(weight_ref[1], frame_ref[0], (1, 1))
    found = []
    start = 0
    for width in widths:
        real = spectra[start : start + width]
        imag = spectra[start + width : start + 2 * width]
        start += 2 * width
        channel = lax.broadcasted_iota(jnp.int32, (width, HALF), 0)
        frame = lax.broadcasted_iota(jnp.int32, (width, HALF), 1)
        sign = jnp.where(channel & frame & 1 == 1, -1.0, 1.0)
        is_odd = channel & 1 == 1
        real_sign = jnp.where(channel & 3 >= 2, -sign, sign)
        imag_sign = jnp.where((channel + 1) & 3 >= 2, -sign, sign)
        found.append((
            real[:, :HALF] * sign,
            imag[:, :HALF] * sign,
            jnp.where(is_odd, imag[:, HALF:], real[:, HALF:]) * real_sign,
            jnp.where(is_odd, real[:, HALF:], imag[:, HALF:]) * imag_sign,
        ))
    return found


def kernel(order, sizes, key_ref, rec_ref, weight_ref, dft_ref, out_ref,
           real_ref, imag_ref, frame_ref, first_ref, second_ref, even_ref, odd_ref, total_ref, sem):
    devices, widths, windows = sizes
    lead_width, trail_width = widths
    block = rec_ref.shape[1] // 2
    rows = devices * block
    pattern = first_ref.shape[1] // lead_width
    height = trail_width * windows
    steps = lead_width // GROUP

    key = key_ref[0]
    for device in range(devices):
        slot = key ^ slot_of(device, order)
        piece = rec_ref[slot]
        real_ref[device * block : (device + 1) * block] = piece[:block]
        imag_ref[device * block : (device + 1) * block] = piece[block:]
    zeros = jnp.zeros((8, LANES), jnp.float32)
    real_ref[rows : rows + 8] = zeros
    imag_ref[rows : rows + 8] = zeros
    for window in range(windows):
        lead, trail = spectra_of(window, widths, real_ref, imag_ref, weight_ref, frame_ref)
        for i in range(4):
            second_ref[i, pl.ds(window, trail_width, stride=windows), :] = trail[i]
            for copy in range(pattern // windows):
                place = pl.ds(copy * windows + window, lead_width, stride=pattern)
                first_ref[i, place, :] = lead[i]

    def multiply(step, z_ref):
        for local in range(GROUP):
            place = pl.ds(pl.multiple_of((step * GROUP + local) * pattern, pattern), pattern)
            lead = [first_ref[i, place, :] for i in range(4)]
            for start in range(0, height, pattern):
                trail = [second_ref[i, start : start + pattern] for i in range(4)]
                row = local * height + start
                for odd in range(2):
                    ar, ai = lead[2 * odd : 2 * odd + 2]
                    br, bi = trail[2 * odd : 2 * odd + 2]
                    for part, value in enumerate((ar * br + ai * bi, ai * br - ar * bi)):
                        high, low = halves(value)
                        column = part * LANES
                        z_ref[odd, 0, row : row + pattern, column : column + LANES] = high
                        z_ref[odd, 1, row : row + pattern, column : column + LANES] = low

    def copy_out(step):
        size = GROUP * height * 4
        place = pl.ds(pl.multiple_of(step * size, size), size)
        return pltpu.make_async_copy(total_ref.at[place], out_ref.at[place], sem.at[step])

    def transform(step, z_ref):
        chunk = min(256, height * GROUP)
        for row in range(0, height * GROUP, chunk):
            sums = []
            for odd in range(2):
                high = z_ref[odd, 0, row : row + chunk]
                low = z_ref[odd, 1, row : row + chunk]
                total = dot(high, dft_ref[odd, 0])
                total += dot(low, dft_ref[odd, 0])
                total += dot(high, dft_ref[odd, 1])
                sums.append(total)
            base = pl.multiple_of((step * GROUP * height + row) * 4, 4 * chunk)
            for i, value in enumerate((sums[0] + sums[1], sums[0] - sums[1])):
                for part in range(2):
                    total_ref[pl.ds(base + 2 * i + part, chunk, stride=4), :] = value[
                        :, part * HALF : (part + 1) * HALF
                    ]
        copy_out(step).start()

    multiply(0, even_ref)

    @pl.loop(0, steps, step=2)
    def _(step):
        multiply(step + 1, odd_ref)
        transform(step, even_ref)
        multiply(jnp.minimum(step + 2, steps - 1), even_ref)
        transform(step + 1, odd_ref)

    for step in range(steps):
        copy_out(step).wait()


def tables(widths, offsets):
    table = jnp.asarray(np.stack(split_table(channel_table())))
    dft = jnp.asarray(np.stack([np.stack(split_table(window_table(odd))) for odd in range(2)]))
    vmem = pl.BlockSpec(memory_space=pltpu.VMEM)
    return pl.pallas_call(
        functools.partial(fetch, widths),
        out_shape=(
            jax.ShapeDtypeStruct((2, 2 * sum(widths), 2 * C), jnp.bfloat16),
            jax.ShapeDtypeStruct(dft.shape, jnp.bfloat16),
        ),
        in_specs=[pl.BlockSpec(memory_space=pltpu.SMEM), vmem, vmem],
        out_specs=(vmem, vmem),
        compiler_params=pltpu.CompilerParams(vmem_limit_bytes=8 * 2**20),
        cost_estimate=pl.CostEstimate(flops=2 * 10**9, bytes_accessed=10**6, transcendentals=0),
    )(offsets, table, dft)


def local(record):
    row_count = lax.axis_size("row")
    col_count = lax.axis_size("col")
    devices = row_count * col_count
    axes = ("row", "col")
    lead_width = C // row_count
    trail_width = C // col_count
    samples = record.shape[1]
    windows = samples * devices // HOP // P_SIZE
    row_index = lax.axis_index("row")
    col_index = lax.axis_index("col")
    me = row_index * col_count + col_index

    col_bits = list(range(col_count.bit_length() - 1))
    row_bits = list(range(len(col_bits), devices.bit_length() - 1))
    order = tuple(col_bits[::-1] + row_bits[1:] + row_bits[:1])
    widths = (lead_width, trail_width)
    offsets = jnp.stack([row_index * lead_width, col_index * trail_width]).astype(jnp.int32)
    weights, dft = tables(widths, offsets)
    blocks = record.reshape(1, 2 * samples // LANES, LANES)
    for stage, bit in enumerate(order):
        if stage == 1:
            blocks, weights, dft = lax.optimization_barrier((blocks, weights, dft))
        route = [(i, i ^ (1 << bit)) for i in range(devices)]
        blocks = jnp.concatenate([blocks, lax.ppermute(blocks, axes, route)], axis=0)

    key = slot_of(me, order).astype(jnp.int32).reshape(1)
    height = trail_width * windows
    pattern = max(8, windows)
    sizes = (devices, widths, windows)
    vmem = pl.BlockSpec(memory_space=pltpu.VMEM)
    smem = pl.BlockSpec(memory_space=pltpu.SMEM)
    out = pl.pallas_call(
        functools.partial(kernel, order, sizes),
        out_shape=jax.ShapeDtypeStruct((lead_width * height * 4, LANES), jnp.float32),
        in_specs=[smem, vmem, vmem, vmem],
        out_specs=pl.BlockSpec(memory_space=pltpu.HBM),
        scratch_shapes=[
            pltpu.VMEM((devices * samples // LANES + 8, LANES), jnp.float32),
            pltpu.VMEM((devices * samples // LANES + 8, LANES), jnp.float32),
            pltpu.VMEM((2, P_SIZE, 2 * C), jnp.bfloat16),
            pltpu.VMEM((4, lead_width * pattern, LANES), jnp.float32),
            pltpu.VMEM((4, height, LANES), jnp.float32),
            pltpu.VMEM((2, 2, GROUP * height, 2 * LANES), jnp.bfloat16),
            pltpu.VMEM((2, 2, GROUP * height, 2 * LANES), jnp.bfloat16),
            pltpu.VMEM((lead_width * height * 4, LANES), jnp.float32),
            pltpu.SemaphoreType.DMA((lead_width // GROUP,)),
        ],
        compiler_params=pltpu.CompilerParams(vmem_limit_bytes=40 * 2**20),
        cost_estimate=pl.CostEstimate(flops=10**10, bytes_accessed=10**7, transcendentals=0),
    )(key, blocks, weights, dft)
    out = out.reshape(lead_width, trail_width, windows, 2, 2, LANES)
    return out.transpose(0, 1, 2, 4, 3, 5).reshape(
        lead_width, trail_width, windows, 2, P_SIZE
    )


def solution(mesh):
    return jax.shard_map(
        local,
        mesh=mesh,
        in_specs=(P(None, ("row", "col")),),
        out_specs=P("row", "col", None, None, None),
        check_vma=False,
    )
```

```python
import functools
import math

import jax
import jax.numpy as jnp
import numpy as np
from jax import lax
from jax.experimental import pallas as pl
from jax.experimental.pallas import tpu as pltpu
from jax.sharding import PartitionSpec as P

C = 256
P_SIZE = 256
HOP = 64
LANES = 128
HALF = P_SIZE // 2
GROUP = 4


def split_table(table):
    high = table.astype(jnp.bfloat16)
    low = (table - high.astype(np.float64)).astype(jnp.bfloat16)
    return high, low


def channel_table():
    m = np.arange(C)
    hann = (0.5 - 0.5 * np.cos(2.0 * math.pi * m / C)) / math.sqrt(3.0 * C / 8.0)
    phase = 2.0 * math.pi * (np.arange(C)[:, None] * m[None, :] % C) / C
    cosine = hann * np.cos(phase)
    sinus = hann * np.sin(phase)
    upper = np.concatenate([cosine, sinus], axis=1)
    lower = np.concatenate([-sinus, cosine], axis=1)
    return np.stack([upper, lower])


def window_table(odd):
    p = 2 * np.arange(HALF) + odd
    phase = 2.0 * math.pi * (p[:, None] * np.arange(HALF)[None, :] % P_SIZE) / P_SIZE
    cosine = np.cos(phase) / math.sqrt(P_SIZE)
    sinus = np.sin(phase) / math.sqrt(P_SIZE)
    upper = np.concatenate([cosine, -sinus], axis=1)
    lower = np.concatenate([sinus, cosine], axis=1)
    return np.concatenate([upper, lower], axis=0)


def halves(x):
    high = x.astype(jnp.bfloat16)
    return high, (x - high.astype(jnp.float32)).astype(jnp.bfloat16)


def dot(a, b, contract=(1, 0)):
    return lax.dot_general(
        a,
        b,
        (((contract[0],), (contract[1],)), ((), ())),
        preferred_element_type=jnp.float32,
    )


def slot_of(index, order):
    return sum(((index >> bit) & 1) << stage for stage, bit in enumerate(order))


def fetch_weights(widths, offset_ref, table_ref, weight_ref, sem):
    copies = []
    start = 0
    for which, width in enumerate(widths):
        offset = pl.multiple_of(offset_ref[which], width)
        for part in range(2):
            copies.append(
                pltpu.make_async_copy(
                    table_ref.at[:, part, pl.ds(offset, width)],
                    weight_ref.at[:, pl.ds(start, width)],
                    sem.at[len(copies)],
                )
            )
            start += width
    for copy in copies:
        copy.start()
    for copy in copies:
        copy.wait()


def fetch_whole(table_ref, copy_ref, sem):
    copy = pltpu.make_async_copy(table_ref, copy_ref, sem)
    copy.start()
    copy.wait()


def spectra_of(window, widths, real_ref, imag_ref, weight_ref, frame_ref):
    lower = lax.broadcasted_iota(jnp.int32, (HALF, LANES), 1) < HOP
    for part, ref in enumerate((real_ref, imag_ref)):
        shifts = [ref[window * HALF + i : window * HALF + i + HALF] for i in range(3)]
        turned = [pltpu.roll(x, HOP, 1) for x in shifts]
        odd = [jnp.where(lower, turned[i], turned[i + 1]) for i in range(2)]
        for start, pieces in ((0, shifts[:2]), (HALF, odd)):
            for i, piece in enumerate(pieces):
                high, low = halves(piece)
                column = (2 * part + i) * LANES
                frame_ref[0, start : start + HALF, column : column + LANES] = high
                frame_ref[1, start : start + HALF, column : column + LANES] = low
    spectra = dot(weight_ref[0], frame_ref[0], (1, 1))
    spectra += dot(weight_ref[0], frame_ref[1], (1, 1))
    spectra += dot(weight_ref[1], frame_ref[0], (1, 1))
    found = []
    start = 0
    for width in widths:
        real = spectra[start : start + width]
        imag = spectra[start + width : start + 2 * width]
        start += 2 * width
        channel = lax.broadcasted_iota(jnp.int32, (width, HALF), 0)
        frame = lax.broadcasted_iota(jnp.int32, (width, HALF), 1)
        sign = jnp.where(channel & frame & 1 == 1, -1.0, 1.0)
        is_odd = channel & 1 == 1
        real_sign = jnp.where(channel & 3 >= 2, -sign, sign)
        imag_sign = jnp.where((channel + 1) & 3 >= 2, -sign, sign)
        found.append((
            real[:, :HALF] * sign,
            imag[:, :HALF] * sign,
            jnp.where(is_odd, imag[:, HALF:], real[:, HALF:]) * real_sign,
            jnp.where(is_odd, real[:, HALF:], imag[:, HALF:]) * imag_sign,
        ))
    return found


def kernel(order, sizes, key_ref, rec_ref, weight_ref, dft_ref, out_ref,
           real_ref, imag_ref, frame_ref, first_ref, second_ref, even_ref, odd_ref, total_ref, sem):
    devices, widths, windows = sizes
    lead_width, trail_width = widths
    block = rec_ref.shape[1] // 2
    rows = devices * block
    pattern = first_ref.shape[1] // lead_width
    height = trail_width * windows
    steps = lead_width // GROUP

    key = key_ref[0]
    for device in range(devices):
        slot = key ^ slot_of(device, order)
        piece = rec_ref[slot]
        real_ref[device * block : (device + 1) * block] = piece[:block]
        imag_ref[device * block : (device + 1) * block] = piece[block:]
    zeros = jnp.zeros((8, LANES), jnp.float32)
    real_ref[rows : rows + 8] = zeros
    imag_ref[rows : rows + 8] = zeros
    for window in range(windows):
        lead, trail = spectra_of(window, widths, real_ref, imag_ref, weight_ref, frame_ref)
        for i in range(4):
            second_ref[i, pl.ds(window, trail_width, stride=windows), :] = trail[i]
            for copy in range(pattern // windows):
                place = pl.ds(copy * windows + window, lead_width, stride=pattern)
                first_ref[i, place, :] = lead[i]

    def multiply(step, z_ref):
        for local in range(GROUP):
            place = pl.ds(pl.multiple_of((step * GROUP + local) * pattern, pattern), pattern)
            lead = [first_ref[i, place, :] for i in range(4)]
            for start in range(0, height, pattern):
                trail = [second_ref[i, start : start + pattern] for i in range(4)]
                row = local * height + start
                for odd in range(2):
                    ar, ai = lead[2 * odd : 2 * odd + 2]
                    br, bi = trail[2 * odd : 2 * odd + 2]
                    for part, value in enumerate((ar * br + ai * bi, ai * br - ar * bi)):
                        high, low = halves(value)
                        column = part * LANES
                        z_ref[odd, 0, row : row + pattern, column : column + LANES] = high
                        z_ref[odd, 1, row : row + pattern, column : column + LANES] = low

    def copy_out(step):
        size = GROUP * height * 4
        place = pl.ds(pl.multiple_of(step * size, size), size)
        return pltpu.make_async_copy(total_ref.at[place], out_ref.at[place], sem.at[step])

    def transform(step, z_ref):
        chunk = min(256, height * GROUP)
        for row in range(0, height * GROUP, chunk):
            sums = []
            for odd in range(2):
                high = z_ref[odd, 0, row : row + chunk]
                low = z_ref[odd, 1, row : row + chunk]
                total = dot(high, dft_ref[odd, 0])
                total += dot(low, dft_ref[odd, 0])
                total += dot(high, dft_ref[odd, 1])
                sums.append(total)
            base = pl.multiple_of((step * GROUP * height + row) * 4, 4 * chunk)
            for i, value in enumerate((sums[0] + sums[1], sums[0] - sums[1])):
                for part in range(2):
                    total_ref[pl.ds(base + 2 * i + part, chunk, stride=4), :] = value[
                        :, part * HALF : (part + 1) * HALF
                    ]
        copy_out(step).start()

    multiply(0, even_ref)

    @pl.loop(0, steps, step=2)
    def _(step):
        multiply(step + 1, odd_ref)
        transform(step, even_ref)
        multiply(jnp.minimum(step + 2, steps - 1), even_ref)
        transform(step + 1, odd_ref)

    for step in range(steps):
        copy_out(step).wait()


def fetched(body, scalars, table, shape, sem):
    return pl.pallas_call(
        body,
        out_shape=jax.ShapeDtypeStruct(shape, table.dtype),
        in_specs=[pl.BlockSpec(memory_space=pltpu.SMEM)] * len(scalars)
        + [pl.BlockSpec(memory_space=pltpu.HBM)],
        out_specs=pl.BlockSpec(memory_space=pltpu.VMEM),
        scratch_shapes=[sem],
        compiler_params=pltpu.CompilerParams(vmem_limit_bytes=8 * 2**20),
        cost_estimate=pl.CostEstimate(flops=10**9, bytes_accessed=10**6, transcendentals=0),
    )(*scalars, pltpu.with_memory_space_constraint(jnp.asarray(table), pltpu.HBM))


def local(record):
    row_count = lax.axis_size("row")
    col_count = lax.axis_size("col")
    devices = row_count * col_count
    axes = ("row", "col")
    lead_width = C // row_count
    trail_width = C // col_count
    samples = record.shape[1]
    windows = samples * devices // HOP // P_SIZE
    row_index = lax.axis_index("row")
    col_index = lax.axis_index("col")
    me = row_index * col_count + col_index

    col_bits = list(range(col_count.bit_length() - 1))
    row_bits = list(range(len(col_bits), devices.bit_length() - 1))
    order = tuple(col_bits[::-1] + row_bits[1:] + row_bits[:1])
    widths = (lead_width, trail_width)
    offsets = jnp.stack([row_index * lead_width, col_index * trail_width]).astype(jnp.int32)
    weights = fetched(
        functools.partial(fetch_weights, widths),
        (offsets,),
        np.stack(split_table(channel_table())),
        (2, 2 * sum(widths), 2 * C),
        pltpu.SemaphoreType.DMA((4,)),
    )
    dft = np.stack([np.stack(split_table(window_table(odd))) for odd in range(2)])
    dft = fetched(fetch_whole, (), dft, dft.shape, pltpu.SemaphoreType.DMA(()))
    blocks = record.reshape(1, 2 * samples // LANES, LANES)
    for stage, bit in enumerate(order):
        if stage == 1:
            blocks, weights = lax.optimization_barrier((blocks, weights))
        if stage == 2:
            blocks, dft = lax.optimization_barrier((blocks, dft))
        route = [(i, i ^ (1 << bit)) for i in range(devices)]
        blocks = jnp.concatenate([blocks, lax.ppermute(blocks, axes, route)], axis=0)

    key = slot_of(me, order).astype(jnp.int32).reshape(1)
    height = trail_width * windows
    pattern = max(8, windows)
    sizes = (devices, widths, windows)
    vmem = pl.BlockSpec(memory_space=pltpu.VMEM)
    smem = pl.BlockSpec(memory_space=pltpu.SMEM)
    out = pl.pallas_call(
        functools.partial(kernel, order, sizes),
        out_shape=jax.ShapeDtypeStruct((lead_width * height * 4, LANES), jnp.float32),
        in_specs=[smem, vmem, vmem, vmem],
        out_specs=pl.BlockSpec(memory_space=pltpu.HBM),
        scratch_shapes=[
            pltpu.VMEM((devices * samples // LANES + 8, LANES), jnp.float32),
            pltpu.VMEM((devices * samples // LANES + 8, LANES), jnp.float32),
            pltpu.VMEM((2, P_SIZE, 2 * C), jnp.bfloat16),
            pltpu.VMEM((4, lead_width * pattern, LANES), jnp.float32),
            pltpu.VMEM((4, height, LANES), jnp.float32),
            pltpu.VMEM((2, 2, GROUP * height, 2 * LANES), jnp.bfloat16),
            pltpu.VMEM((2, 2, GROUP * height, 2 * LANES), jnp.bfloat16),
            pltpu.VMEM((lead_width * height * 4, LANES), jnp.float32),
            pltpu.SemaphoreType.DMA((lead_width // GROUP,)),
        ],
        compiler_params=pltpu.CompilerParams(vmem_limit_bytes=40 * 2**20),
        cost_estimate=pl.CostEstimate(flops=10**10, bytes_accessed=10**7, transcendentals=0),
    )(key, blocks, weights, dft)
    out = out.reshape(lead_width, trail_width, windows, 2, 2, LANES)
    return out.transpose(0, 1, 2, 4, 3, 5).reshape(
        lead_width, trail_width, windows, 2, P_SIZE
    )


def solution(mesh):
    return jax.shard_map(
        local,
        mesh=mesh,
        in_specs=(P(None, ("row", "col")),),
        out_specs=P("row", "col", None, None, None),
        check_vma=False,
    )
```

```python
import functools
import math

import jax
import jax.numpy as jnp
import numpy as np
from jax import lax
from jax.experimental import pallas as pl
from jax.experimental.pallas import tpu as pltpu
from jax.sharding import PartitionSpec as P

C = 256
P_SIZE = 256
HOP = 64
LANES = 128
SUBLANES = 8
HALF = P_SIZE // 2
GROUP = 2


def split_table(table):
    high = table.astype(jnp.bfloat16)
    low = (table - high.astype(np.float64)).astype(jnp.bfloat16)
    return high, low


def channel_table():
    m = np.arange(C)
    hann = (0.5 - 0.5 * np.cos(2.0 * math.pi * m / C)) / math.sqrt(3.0 * C / 8.0)
    phase = 2.0 * math.pi * (np.arange(C)[:, None] * m[None, :] % C) / C
    cosine = hann * np.cos(phase)
    sinus = hann * np.sin(phase)
    upper = np.concatenate([cosine, sinus], axis=1)
    lower = np.concatenate([-sinus, cosine], axis=1)
    return np.stack([upper, lower])


def window_table(odd):
    p = 2 * np.arange(HALF) + odd
    phase = 2.0 * math.pi * (p[:, None] * np.arange(HALF)[None, :] % P_SIZE) / P_SIZE
    cosine = np.cos(phase) / math.sqrt(P_SIZE)
    sinus = np.sin(phase) / math.sqrt(P_SIZE)
    upper = np.concatenate([cosine, -sinus], axis=1)
    lower = np.concatenate([sinus, cosine], axis=1)
    return np.concatenate([upper, lower], axis=0)


def dot(a, b, contract=(1, 0)):
    return lax.dot_general(
        a,
        b,
        (((contract[0],), (contract[1],)), ((), ())),
        preferred_element_type=jnp.float32,
    )


def slot_of(index, order):
    return sum(((index >> bit) & 1) << stage for stage, bit in enumerate(order))


def fetch_weights(widths, offset_ref, table_ref, weight_ref, held_ref, sem):
    copies = []
    start = 0
    for which, width in enumerate(widths):
        offset = pl.multiple_of(offset_ref[which], width)
        for part in range(2):
            copies.append(
                pltpu.make_async_copy(
                    table_ref.at[:, part, pl.ds(offset, width)],
                    held_ref.at[:, pl.ds(start, width)],
                    sem.at[len(copies)],
                )
            )
            start += width
    for copy in copies:
        copy.start()
    for copy in copies:
        copy.wait()
    weight_ref[...] = held_ref[...].astype(jnp.float32)


def fetch_whole(table_ref, whole_ref, held_ref, sem):
    copy = pltpu.make_async_copy(table_ref, held_ref, sem.at[0])
    copy.start()
    copy.wait()
    whole_ref[...] = held_ref[...].astype(jnp.float32)


def rounded_off(x):
    return x - x.astype(jnp.bfloat16).astype(jnp.float32)


def spectra_of(window, widths, sample_ref, weight_ref):
    def frames(low):
        return jnp.concatenate([
            jnp.concatenate([
                sample_ref[part, odd, low, window * HALF + i : window * HALF + i + HALF]
                for part in range(2)
                for i in range(2)
            ], axis=1)
            for odd in range(2)
        ])
    count = 2 * sum(widths)
    both = dot(weight_ref[...].reshape(2 * count, 2 * C), frames(0), (1, 1))
    spectra = both[:count] + both[count:]
    spectra += dot(weight_ref[0], frames(1), (1, 1))
    found = []
    start = 0
    for width in widths:
        real = spectra[start : start + width]
        imag = spectra[start + width : start + 2 * width]
        start += 2 * width
        channel = lax.broadcasted_iota(jnp.int32, (width, HALF), 0)
        frame = lax.broadcasted_iota(jnp.int32, (width, HALF), 1)
        sign = jnp.where(channel & frame & 1 == 1, -1.0, 1.0)
        is_odd = channel & 1 == 1
        real_sign = jnp.where(channel & 3 >= 2, -sign, sign)
        imag_sign = jnp.where((channel + 1) & 3 >= 2, -sign, sign)
        found.append((
            real[:, :HALF] * sign,
            imag[:, :HALF] * sign,
            jnp.where(is_odd, imag[:, HALF:], real[:, HALF:]) * real_sign,
            jnp.where(is_odd, real[:, HALF:], imag[:, HALF:]) * imag_sign,
        ))
    return found


def kernel(order, sizes, key_ref, rec_ref, weight_ref, dft_ref, out_ref,
           sample_ref, first_ref, second_ref, even_ref, odd_ref, total_ref, sem):
    devices, widths, windows = sizes
    lead_width, trail_width = widths
    block = rec_ref.shape[1] // 2
    rows = devices * block
    pattern = first_ref.shape[1] // lead_width
    height = trail_width * windows
    steps = lead_width // GROUP

    key = key_ref[0]
    for device in range(devices):
        piece = rec_ref[key ^ slot_of(device, order)]
        for part in range(2):
            place = slice(device * block, (device + 1) * block)
            sample_ref[part, 0, 0, place] = piece[part * block : (part + 1) * block]
    lower = lax.broadcasted_iota(jnp.int32, (rows, LANES), 1) < HOP
    zeros = jnp.zeros((SUBLANES, LANES), jnp.float32)
    for part in range(2):
        sample_ref[part, 0, 0, rows:] = zeros
        turned = [
            pltpu.roll(sample_ref[part, 0, 0, i : i + rows], HOP, 1) for i in range(2)
        ]
        sample_ref[part, 1, 0, :rows] = jnp.where(lower, turned[0], turned[1])
        sample_ref[part, 1, 0, rows:] = zeros
        for odd in range(2):
            sample_ref[part, odd, 1] = rounded_off(sample_ref[part, odd, 0])
    for window in range(windows):
        lead, trail = spectra_of(window, widths, sample_ref, weight_ref)
        for i in range(4):
            second_ref[i, pl.ds(window, trail_width, stride=windows), :] = trail[i]
            for copy in range(pattern // windows):
                place = pl.ds(copy * windows + window, lead_width, stride=pattern)
                first_ref[i, place, :] = lead[i]

    def multiply(step, z_ref):
        for local in range(GROUP):
            place = pl.ds(pl.multiple_of((step * GROUP + local) * pattern, pattern), pattern)
            lead = [first_ref[i, place, :] for i in range(4)]
            for start in range(0, height, pattern):
                trail = [second_ref[i, start : start + pattern] for i in range(4)]
                row = local * height + start
                for odd in range(2):
                    ar, ai = lead[2 * odd : 2 * odd + 2]
                    br, bi = trail[2 * odd : 2 * odd + 2]
                    for part, value in enumerate((ar * br + ai * bi, ai * br - ar * bi)):
                        column = part * LANES
                        z_ref[odd, 0, row : row + pattern, column : column + LANES] = value
                        z_ref[odd, 1, row : row + pattern, column : column + LANES] = rounded_off(value)

    def copy_out(step):
        size = GROUP * height * 4
        place = pl.ds(pl.multiple_of(step * size, size), size)
        return pltpu.make_async_copy(total_ref.at[place], out_ref.at[place], sem.at[step])

    def transform(step, z_ref):
        chunk = min(256, height * GROUP)
        for row in range(0, height * GROUP, chunk):
            sums = []
            for odd in range(2):
                high = z_ref[odd, 0, row : row + chunk]
                low = z_ref[odd, 1, row : row + chunk]
                total = dot(high, dft_ref[odd, 0])
                total += dot(low, dft_ref[odd, 0])
                total += dot(high, dft_ref[odd, 1])
                sums.append(total)
            base = pl.multiple_of((step * GROUP * height + row) * 4, 4 * chunk)
            for i, value in enumerate((sums[0] + sums[1], sums[0] - sums[1])):
                for part in range(2):
                    total_ref[pl.ds(base + 2 * i + part, chunk, stride=4), :] = value[
                        :, part * HALF : (part + 1) * HALF
                    ]
        copy_out(step).start()

    refs = (even_ref, odd_ref)
    multiply(0, even_ref)

    for step in range(steps):
        if step + 1 < steps:
            multiply(step + 1, refs[(step + 1) % 2])
        transform(step, refs[step % 2])

    for step in range(steps):
        copy_out(step).wait()


def fetched(body, scalars, table, shape):
    return pl.pallas_call(
        body,
        out_shape=jax.ShapeDtypeStruct(shape, jnp.float32),
        in_specs=[pl.BlockSpec(memory_space=pltpu.SMEM)] * len(scalars)
        + [pl.BlockSpec(memory_space=pltpu.HBM)],
        out_specs=pl.BlockSpec(memory_space=pltpu.VMEM),
        scratch_shapes=[pltpu.VMEM(shape, jnp.bfloat16), pltpu.SemaphoreType.DMA((4,))],
        compiler_params=pltpu.CompilerParams(vmem_limit_bytes=8 * 2**20),
        cost_estimate=pl.CostEstimate(flops=10**9, bytes_accessed=10**6, transcendentals=0),
    )(*scalars, pltpu.with_memory_space_constraint(jnp.asarray(table), pltpu.HBM))


def local(record):
    row_count = lax.axis_size("row")
    col_count = lax.axis_size("col")
    devices = row_count * col_count
    axes = ("row", "col")
    lead_width = C // row_count
    trail_width = C // col_count
    samples = record.shape[1]
    windows = samples * devices // HOP // P_SIZE
    row_index = lax.axis_index("row")
    col_index = lax.axis_index("col")
    me = row_index * col_count + col_index

    col_bits = list(range(col_count.bit_length() - 1))
    row_bits = list(range(len(col_bits), devices.bit_length() - 1))
    order = tuple(col_bits[::-1] + row_bits[1:] + row_bits[:1])
    widths = (lead_width, trail_width)
    offsets = jnp.stack([row_index * lead_width, col_index * trail_width]).astype(jnp.int32)
    weights = fetched(
        functools.partial(fetch_weights, widths),
        (offsets,),
        np.stack(split_table(channel_table())),
        (2, 2 * sum(widths), 2 * C),
    )
    dft = np.stack([np.stack(split_table(window_table(odd))) for odd in range(2)])
    dft = fetched(fetch_whole, (), dft, dft.shape)
    blocks = record.reshape(1, 2 * samples // LANES, LANES)
    for stage, bit in enumerate(order):
        if stage == 1:
            blocks, dft = lax.optimization_barrier((blocks, dft))
        if stage == 2:
            blocks, weights = lax.optimization_barrier((blocks, weights))
        route = [(i, i ^ (1 << bit)) for i in range(devices)]
        blocks = jnp.concatenate([blocks, lax.ppermute(blocks, axes, route)], axis=0)

    key = slot_of(me, order).astype(jnp.int32).reshape(1)
    height = trail_width * windows
    pattern = max(8, windows)
    sizes = (devices, widths, windows)
    vmem = pl.BlockSpec(memory_space=pltpu.VMEM)
    smem = pl.BlockSpec(memory_space=pltpu.SMEM)
    out = pl.pallas_call(
        functools.partial(kernel, order, sizes),
        out_shape=jax.ShapeDtypeStruct((lead_width * height * 4, LANES), jnp.float32),
        in_specs=[smem, vmem, vmem, vmem],
        out_specs=pl.BlockSpec(memory_space=pltpu.HBM),
        scratch_shapes=[
            pltpu.VMEM((2, 2, 2, devices * samples // LANES + SUBLANES, LANES), jnp.float32),
            pltpu.VMEM((4, lead_width * pattern, LANES), jnp.float32),
            pltpu.VMEM((4, height, LANES), jnp.float32),
            pltpu.VMEM((2, 2, GROUP * height, 2 * LANES), jnp.float32),
            pltpu.VMEM((2, 2, GROUP * height, 2 * LANES), jnp.float32),
            pltpu.VMEM((lead_width * height * 4, LANES), jnp.float32),
            pltpu.SemaphoreType.DMA((lead_width // GROUP,)),
        ],
        compiler_params=pltpu.CompilerParams(vmem_limit_bytes=40 * 2**20),
        cost_estimate=pl.CostEstimate(flops=10**10, bytes_accessed=10**7, transcendentals=0),
    )(key, blocks, weights, dft)
    out = out.reshape(lead_width, trail_width, windows, 2, 2, LANES)
    return out.transpose(0, 1, 2, 4, 3, 5).reshape(
        lead_width, trail_width, windows, 2, P_SIZE
    )


def solution(mesh):
    return jax.shard_map(
        local,
        mesh=mesh,
        in_specs=(P(None, ("row", "col")),),
        out_specs=P("row", "col", None, None, None),
        check_vma=False,
    )
```

```python
import functools
import math

import jax
import jax.numpy as jnp
import numpy as np
from jax import lax
from jax.experimental import pallas as pl
from jax.experimental.pallas import tpu as pltpu
from jax.sharding import PartitionSpec as P

C = 256
P_SIZE = 256
HOP = 64
LANES = 128
SUBLANES = 8
HALF = P_SIZE // 2
GROUP = 2


def split_table(table):
    high = table.astype(jnp.bfloat16)
    low = (table - high.astype(np.float64)).astype(jnp.bfloat16)
    return high, low


def channel_table():
    m = np.arange(C)
    hann = (0.5 - 0.5 * np.cos(2.0 * math.pi * m / C)) / math.sqrt(3.0 * C / 8.0)
    phase = 2.0 * math.pi * (np.arange(C)[:, None] * m[None, :] % C) / C
    cosine = hann * np.cos(phase)
    sinus = hann * np.sin(phase)
    upper = np.concatenate([cosine, sinus], axis=1)
    lower = np.concatenate([-sinus, cosine], axis=1)
    return np.stack([upper, lower])


def window_table(odd):
    p = 2 * np.arange(HALF) + odd
    phase = 2.0 * math.pi * (p[:, None] * np.arange(HALF)[None, :] % P_SIZE) / P_SIZE
    cosine = np.cos(phase) / math.sqrt(P_SIZE)
    sinus = np.sin(phase) / math.sqrt(P_SIZE)
    upper = np.concatenate([cosine, -sinus], axis=1)
    lower = np.concatenate([sinus, cosine], axis=1)
    return np.concatenate([upper, lower], axis=0)


def dot(a, b, contract=(1, 0)):
    return lax.dot_general(
        a,
        b,
        (((contract[0],), (contract[1],)), ((), ())),
        preferred_element_type=jnp.float32,
    )


def slot_of(index, order):
    return sum(((index >> bit) & 1) << stage for stage, bit in enumerate(order))


def fetch_weights(widths, offset_ref, table_ref, weight_ref, held_ref, sem):
    copies = []
    start = 0
    for which, width in enumerate(widths):
        offset = pl.multiple_of(offset_ref[which], width)
        for part in range(2):
            copies.append(
                pltpu.make_async_copy(
                    table_ref.at[:, part, pl.ds(offset, width)],
                    held_ref.at[:, pl.ds(start, width)],
                    sem.at[len(copies)],
                )
            )
            start += width
    for copy in copies:
        copy.start()
    for copy in copies:
        copy.wait()
    weight_ref[...] = held_ref[...].astype(jnp.float32)


def fetch_whole(own_ref, table_ref, own_copy_ref, whole_ref, held_ref, sem):
    copies = [
        pltpu.make_async_copy(own_ref, own_copy_ref, sem.at[0]),
        pltpu.make_async_copy(table_ref, held_ref, sem.at[1]),
    ]
    for copy in copies:
        copy.start()
    for copy in copies:
        copy.wait()
    whole_ref[...] = held_ref[...].astype(jnp.float32)


def rounded_off(x):
    return x - x.astype(jnp.bfloat16).astype(jnp.float32)


def spectra_of(window, widths, sample_ref, weight_ref):
    def frames(low):
        return jnp.concatenate([
            jnp.concatenate([
                sample_ref[part, odd, low, window * HALF + i : window * HALF + i + HALF]
                for part in range(2)
                for i in range(2)
            ], axis=1)
            for odd in range(2)
        ])
    count = 2 * sum(widths)
    both = dot(weight_ref[...].reshape(2 * count, 2 * C), frames(0), (1, 1))
    spectra = both[:count] + both[count:]
    spectra += dot(weight_ref[0], frames(1), (1, 1))
    found = []
    start = 0
    for width in widths:
        real = spectra[start : start + width]
        imag = spectra[start + width : start + 2 * width]
        start += 2 * width
        channel = lax.broadcasted_iota(jnp.int32, (width, HALF), 0)
        frame = lax.broadcasted_iota(jnp.int32, (width, HALF), 1)
        sign = jnp.where(channel & frame & 1 == 1, -1.0, 1.0)
        is_odd = channel & 1 == 1
        real_sign = jnp.where(channel & 3 >= 2, -sign, sign)
        imag_sign = jnp.where((channel + 1) & 3 >= 2, -sign, sign)
        found.append((
            real[:, :HALF] * sign,
            imag[:, :HALF] * sign,
            jnp.where(is_odd, imag[:, HALF:], real[:, HALF:]) * real_sign,
            jnp.where(is_odd, real[:, HALF:], imag[:, HALF:]) * imag_sign,
        ))
    return found


def kernel(order, sizes, key_ref, rec_ref, weight_ref, dft_ref, out_ref,
           sample_ref, first_ref, second_ref, even_ref, odd_ref, total_ref, sem):
    devices, widths, windows = sizes
    lead_width, trail_width = widths
    block = rec_ref.shape[1] // 2
    rows = devices * block
    pattern = first_ref.shape[1] // lead_width
    height = trail_width * windows
    steps = lead_width // GROUP

    key = key_ref[0]
    for device in range(devices):
        slot = key ^ slot_of(device, order)
        for part in range(2):
            place = slice(device * block, (device + 1) * block)
            sample_ref[part, 0, 0, place] = rec_ref[slot, pl.ds(part, block, stride=2), :]
    lower = lax.broadcasted_iota(jnp.int32, (rows, LANES), 1) < HOP
    zeros = jnp.zeros((SUBLANES, LANES), jnp.float32)
    for part in range(2):
        sample_ref[part, 0, 0, rows:] = zeros
        turned = [
            pltpu.roll(sample_ref[part, 0, 0, i : i + rows], HOP, 1) for i in range(2)
        ]
        sample_ref[part, 1, 0, :rows] = jnp.where(lower, turned[0], turned[1])
        sample_ref[part, 1, 0, rows:] = zeros
        for odd in range(2):
            sample_ref[part, odd, 1] = rounded_off(sample_ref[part, odd, 0])
    for window in range(windows):
        lead, trail = spectra_of(window, widths, sample_ref, weight_ref)
        for i in range(4):
            second_ref[i, pl.ds(window, trail_width, stride=windows), :] = trail[i]
            for copy in range(pattern // windows):
                place = pl.ds(copy * windows + window, lead_width, stride=pattern)
                first_ref[i, place, :] = lead[i]

    def multiply(step, z_ref):
        for local in range(GROUP):
            place = pl.ds(pl.multiple_of((step * GROUP + local) * pattern, pattern), pattern)
            lead = [first_ref[i, place, :] for i in range(4)]
            for start in range(0, height, pattern):
                trail = [second_ref[i, start : start + pattern] for i in range(4)]
                row = local * height + start
                for odd in range(2):
                    ar, ai = lead[2 * odd : 2 * odd + 2]
                    br, bi = trail[2 * odd : 2 * odd + 2]
                    for part, value in enumerate((ar * br + ai * bi, ai * br - ar * bi)):
                        column = part * LANES
                        z_ref[odd, 0, row : row + pattern, column : column + LANES] = value
                        z_ref[odd, 1, row : row + pattern, column : column + LANES] = rounded_off(value)

    def copy_out(step):
        size = GROUP * height * 4
        place = pl.ds(pl.multiple_of(step * size, size), size)
        return pltpu.make_async_copy(total_ref.at[place], out_ref.at[place], sem.at[step])

    def transform(step, z_ref):
        chunk = min(256, height * GROUP)
        for row in range(0, height * GROUP, chunk):
            sums = []
            for odd in range(2):
                high = z_ref[odd, 0, row : row + chunk]
                low = z_ref[odd, 1, row : row + chunk]
                total = dot(low, dft_ref[odd, 0])
                total += dot(high, dft_ref[odd, 0])
                total += dot(high, dft_ref[odd, 1])
                sums.append(total)
            base = pl.multiple_of((step * GROUP * height + row) * 4, 4 * chunk)
            for i, value in enumerate((sums[0] + sums[1], sums[0] - sums[1])):
                for part in range(2):
                    total_ref[pl.ds(base + 2 * i + part, chunk, stride=4), :] = value[
                        :, part * HALF : (part + 1) * HALF
                    ]
        copy_out(step).start()

    refs = (even_ref, odd_ref)
    multiply(0, even_ref)

    for step in range(steps):
        if step + 1 < steps:
            multiply(step + 1, refs[(step + 1) % 2])
        transform(step, refs[step % 2])

    for step in range(steps):
        copy_out(step).wait()


def fetched(body, scalars, arrays, shapes, table):
    vmem = pl.BlockSpec(memory_space=pltpu.VMEM)
    in_hbm = [pltpu.with_memory_space_constraint(x, pltpu.HBM) for x in (*arrays, jnp.asarray(table))]
    return pl.pallas_call(
        body,
        out_shape=[jax.ShapeDtypeStruct(shape, jnp.float32) for shape in shapes],
        in_specs=[pl.BlockSpec(memory_space=pltpu.SMEM)] * len(scalars)
        + [pl.BlockSpec(memory_space=pltpu.HBM)] * len(in_hbm),
        out_specs=[vmem] * len(shapes),
        scratch_shapes=[pltpu.VMEM(shapes[-1], jnp.bfloat16), pltpu.SemaphoreType.DMA((4,))],
        compiler_params=pltpu.CompilerParams(vmem_limit_bytes=8 * 2**20),
        cost_estimate=pl.CostEstimate(flops=10**9, bytes_accessed=10**6, transcendentals=0),
    )(*scalars, *in_hbm)


def local(record):
    row_count = lax.axis_size("row")
    col_count = lax.axis_size("col")
    devices = row_count * col_count
    axes = ("row", "col")
    lead_width = C // row_count
    trail_width = C // col_count
    samples = record.shape[1]
    windows = samples * devices // HOP // P_SIZE
    row_index = lax.axis_index("row")
    col_index = lax.axis_index("col")
    me = row_index * col_count + col_index

    col_bits = list(range(col_count.bit_length() - 1))
    row_bits = list(range(len(col_bits), devices.bit_length() - 1))
    order = tuple(col_bits[::-1] + row_bits[1:] + row_bits[:1])
    widths = (lead_width, trail_width)
    offsets = jnp.stack([row_index * lead_width, col_index * trail_width]).astype(jnp.int32)
    [weights] = fetched(
        functools.partial(fetch_weights, widths),
        (offsets,),
        (),
        [(2, 2 * sum(widths), 2 * C)],
        np.stack(split_table(channel_table())),
    )
    own = record.reshape(2, samples // LANES, LANES).transpose(1, 0, 2)
    own = own.reshape(1, 2 * samples // LANES, LANES)
    dft = np.stack([np.stack(split_table(window_table(odd))) for odd in range(2)])
    blocks, dft = fetched(fetch_whole, (), (own,), [own.shape, dft.shape], dft)
    for stage, bit in enumerate(order):
        route = [(i, i ^ (1 << bit)) for i in range(devices)]
        received = lax.ppermute(blocks if stage else own, axes, route)
        blocks = jnp.concatenate([blocks, received], axis=0)
        if stage == 0:
            blocks, dft = lax.optimization_barrier((blocks, dft))
        if stage == 1:
            blocks, weights = lax.optimization_barrier((blocks, weights))

    key = slot_of(me, order).astype(jnp.int32).reshape(1)
    height = trail_width * windows
    pattern = max(8, windows)
    sizes = (devices, widths, windows)
    vmem = pl.BlockSpec(memory_space=pltpu.VMEM)
    smem = pl.BlockSpec(memory_space=pltpu.SMEM)
    out = pl.pallas_call(
        functools.partial(kernel, order, sizes),
        out_shape=jax.ShapeDtypeStruct((lead_width * height * 4, LANES), jnp.float32),
        in_specs=[smem, vmem, vmem, vmem],
        out_specs=pl.BlockSpec(memory_space=pltpu.HBM),
        scratch_shapes=[
            pltpu.VMEM((2, 2, 2, devices * samples // LANES + SUBLANES, LANES), jnp.float32),
            pltpu.VMEM((4, lead_width * pattern, LANES), jnp.float32),
            pltpu.VMEM((4, height, LANES), jnp.float32),
            pltpu.VMEM((2, 2, GROUP * height, 2 * LANES), jnp.float32),
            pltpu.VMEM((2, 2, GROUP * height, 2 * LANES), jnp.float32),
            pltpu.VMEM((lead_width * height * 4, LANES), jnp.float32),
            pltpu.SemaphoreType.DMA((lead_width // GROUP,)),
        ],
        compiler_params=pltpu.CompilerParams(vmem_limit_bytes=40 * 2**20),
        cost_estimate=pl.CostEstimate(flops=10**10, bytes_accessed=10**7, transcendentals=0),
    )(key, blocks, weights, dft)
    out = out.reshape(lead_width, trail_width, windows, 2, 2, LANES)
    return out.transpose(0, 1, 2, 4, 3, 5).reshape(
        lead_width, trail_width, windows, 2, P_SIZE
    )


def solution(mesh):
    return jax.shard_map(
        local,
        mesh=mesh,
        in_specs=(P(None, ("row", "col")),),
        out_specs=P("row", "col", None, None, None),
        check_vma=False,
    )
```

```python
import functools
import math

import jax
import jax.numpy as jnp
import numpy as np
from jax import lax
from jax.experimental import pallas as pl
from jax.experimental.pallas import tpu as pltpu
from jax.sharding import PartitionSpec as P

C = 256
P_SIZE = 256
HOP = 64
LANES = 128
SUBLANES = 8
HALF = P_SIZE // 2
GROUP = 2


def split_table(table):
    high = table.astype(jnp.bfloat16)
    low = (table - high.astype(np.float64)).astype(jnp.bfloat16)
    return high, low


def channel_table():
    m = np.arange(C)
    hann = (0.5 - 0.5 * np.cos(2.0 * math.pi * m / C)) / math.sqrt(3.0 * C / 8.0)
    phase = 2.0 * math.pi * (np.arange(C)[:, None] * m[None, :] % C) / C
    cosine = hann * np.cos(phase)
    sinus = hann * np.sin(phase)
    upper = np.concatenate([cosine, sinus], axis=1)
    lower = np.concatenate([-sinus, cosine], axis=1)
    return np.stack([upper, lower])


def window_table(odd):
    p = 2 * np.arange(HALF) + odd
    phase = 2.0 * math.pi * (p[:, None] * np.arange(HALF)[None, :] % P_SIZE) / P_SIZE
    cosine = np.cos(phase) / math.sqrt(P_SIZE)
    sinus = np.sin(phase) / math.sqrt(P_SIZE)
    upper = np.concatenate([cosine, -sinus], axis=1)
    lower = np.concatenate([sinus, cosine], axis=1)
    return np.concatenate([upper, lower], axis=0)


def dot(a, b, contract=(1, 0)):
    return lax.dot_general(
        a,
        b,
        (((contract[0],), (contract[1],)), ((), ())),
        preferred_element_type=jnp.float32,
    )


def slot_of(index, order):
    return sum(((index >> bit) & 1) << stage for stage, bit in enumerate(order))


def fetch_weights(widths, offset_ref, table_ref, weight_ref, held_ref, sem):
    copies = []
    start = 0
    for which, width in enumerate(widths):
        offset = pl.multiple_of(offset_ref[which], width)
        for part in range(2):
            copies.append(
                pltpu.make_async_copy(
                    table_ref.at[:, part, pl.ds(offset, width)],
                    held_ref.at[:, pl.ds(start, width)],
                    sem.at[len(copies)],
                )
            )
            start += width
    for copy in copies:
        copy.start()
    for copy in copies:
        copy.wait()
    weight_ref[...] = held_ref[...].astype(jnp.float32)


def fetch_whole(own_ref, table_ref, own_copy_ref, whole_ref, held_ref, sem):
    copies = [
        pltpu.make_async_copy(own_ref, own_copy_ref, sem.at[0]),
        pltpu.make_async_copy(table_ref, held_ref, sem.at[1]),
    ]
    for copy in copies:
        copy.start()
    for copy in copies:
        copy.wait()
    whole_ref[...] = held_ref[...].astype(jnp.float32)


def rounded_off(x):
    return x - x.astype(jnp.bfloat16).astype(jnp.float32)


def spectra_of(window, widths, sample_ref, weight_ref):
    def frames(low):
        return jnp.concatenate([
            jnp.concatenate([
                sample_ref[part, odd, low, window * HALF + i : window * HALF + i + HALF]
                for part in range(2)
                for i in range(2)
            ], axis=1)
            for odd in range(2)
        ])
    count = 2 * sum(widths)
    both = dot(weight_ref[...].reshape(2 * count, 2 * C), frames(0), (1, 1))
    spectra = both[:count] + both[count:]
    spectra += dot(weight_ref[0], frames(1), (1, 1))
    found = []
    start = 0
    for width in widths:
        real = spectra[start : start + width]
        imag = spectra[start + width : start + 2 * width]
        start += 2 * width
        channel = lax.broadcasted_iota(jnp.int32, (width, HALF), 0)
        frame = lax.broadcasted_iota(jnp.int32, (width, HALF), 1)
        sign = jnp.where(channel & frame & 1 == 1, -1.0, 1.0)
        is_odd = channel & 1 == 1
        real_sign = jnp.where(channel & 3 >= 2, -sign, sign)
        imag_sign = jnp.where((channel + 1) & 3 >= 2, -sign, sign)
        found.append((
            real[:, :HALF] * sign,
            imag[:, :HALF] * sign,
            jnp.where(is_odd, imag[:, HALF:], real[:, HALF:]) * real_sign,
            jnp.where(is_odd, real[:, HALF:], imag[:, HALF:]) * imag_sign,
        ))
    return found


def kernel(order, sizes, key_ref, rec_ref, weight_ref, dft_ref, out_ref,
           sample_ref, first_ref, second_ref, even_ref, odd_ref, total_ref, sem):
    devices, widths, windows = sizes
    lead_width, trail_width = widths
    block = rec_ref.shape[1] // 2
    rows = devices * block
    pattern = first_ref.shape[1] // lead_width
    height = trail_width * windows
    steps = lead_width // GROUP

    key = key_ref[0]
    for device in range(devices):
        slot = key ^ slot_of(device, order)
        for part in range(2):
            place = slice(device * block, (device + 1) * block)
            sample_ref[part, 0, 0, place] = rec_ref[slot, pl.ds(part, block, stride=2), :]
    lower = lax.broadcasted_iota(jnp.int32, (rows, LANES), 1) < HOP
    zeros = jnp.zeros((SUBLANES, LANES), jnp.float32)
    for part in range(2):
        sample_ref[part, 0, 0, rows:] = zeros
        turned = [
            pltpu.roll(sample_ref[part, 0, 0, i : i + rows], HOP, 1) for i in range(2)
        ]
        sample_ref[part, 1, 0, :rows] = jnp.where(lower, turned[0], turned[1])
        sample_ref[part, 1, 0, rows:] = zeros
        for odd in range(2):
            sample_ref[part, odd, 1] = rounded_off(sample_ref[part, odd, 0])
    for window in range(windows):
        lead, trail = spectra_of(window, widths, sample_ref, weight_ref)
        for i in range(4):
            second_ref[i, pl.ds(window, trail_width, stride=windows), :] = trail[i]
            for copy in range(pattern // windows):
                place = pl.ds(copy * windows + window, lead_width, stride=pattern)
                first_ref[i, place, :] = lead[i]

    def multiply(step, z_ref):
        for local in range(GROUP):
            place = pl.ds(pl.multiple_of((step * GROUP + local) * pattern, pattern), pattern)
            lead = [first_ref[i, place, :] for i in range(4)]
            for start in range(0, height, pattern):
                trail = [second_ref[i, start : start + pattern] for i in range(4)]
                row = local * height + start
                for odd in range(2):
                    ar, ai = lead[2 * odd : 2 * odd + 2]
                    br, bi = trail[2 * odd : 2 * odd + 2]
                    for part, value in enumerate((ar * br + ai * bi, ai * br - ar * bi)):
                        column = part * LANES
                        z_ref[odd, 0, row : row + pattern, column : column + LANES] = value
                        z_ref[odd, 1, row : row + pattern, column : column + LANES] = rounded_off(value)

    def copy_out(step):
        size = GROUP * height * 4
        place = pl.ds(pl.multiple_of(step * size, size), size)
        return pltpu.make_async_copy(total_ref.at[place], out_ref.at[place], sem.at[step])

    def transform(step, z_ref):
        chunk = min(256, height * GROUP)
        for row in range(0, height * GROUP, chunk):
            sums = []
            for odd in range(2):
                high = z_ref[odd, 0, row : row + chunk]
                low = z_ref[odd, 1, row : row + chunk]
                total = dot(low, dft_ref[odd, 0])
                total += dot(high, dft_ref[odd, 0])
                total += dot(high, dft_ref[odd, 1])
                sums.append(total)
            base = pl.multiple_of((step * GROUP * height + row) * 4, 4 * chunk)
            for i, value in enumerate((sums[0] + sums[1], sums[0] - sums[1])):
                for part in range(2):
                    total_ref[pl.ds(base + 2 * i + part, chunk, stride=4), :] = value[
                        :, part * HALF : (part + 1) * HALF
                    ]
        copy_out(step).start()

    refs = (even_ref, odd_ref)
    multiply(0, even_ref)

    for step in range(steps):
        transform(step, refs[step % 2])
        if step + 1 < steps:
            multiply(step + 1, refs[(step + 1) % 2])

    for step in range(steps):
        copy_out(step).wait()


def fetched(body, scalars, arrays, shapes, table):
    vmem = pl.BlockSpec(memory_space=pltpu.VMEM)
    in_hbm = [pltpu.with_memory_space_constraint(x, pltpu.HBM) for x in (*arrays, jnp.asarray(table))]
    return pl.pallas_call(
        body,
        out_shape=[jax.ShapeDtypeStruct(shape, jnp.float32) for shape in shapes],
        in_specs=[pl.BlockSpec(memory_space=pltpu.SMEM)] * len(scalars)
        + [pl.BlockSpec(memory_space=pltpu.HBM)] * len(in_hbm),
        out_specs=[vmem] * len(shapes),
        scratch_shapes=[pltpu.VMEM(shapes[-1], jnp.bfloat16), pltpu.SemaphoreType.DMA((4,))],
        compiler_params=pltpu.CompilerParams(vmem_limit_bytes=8 * 2**20),
        cost_estimate=pl.CostEstimate(flops=10**9, bytes_accessed=10**6, transcendentals=0),
    )(*scalars, *in_hbm)


def local(record):
    row_count = lax.axis_size("row")
    col_count = lax.axis_size("col")
    devices = row_count * col_count
    axes = ("row", "col")
    lead_width = C // row_count
    trail_width = C // col_count
    samples = record.shape[1]
    windows = samples * devices // HOP // P_SIZE
    row_index = lax.axis_index("row")
    col_index = lax.axis_index("col")
    me = row_index * col_count + col_index

    col_bits = list(range(col_count.bit_length() - 1))
    row_bits = list(range(len(col_bits), devices.bit_length() - 1))
    order = tuple(col_bits[::-1] + row_bits[1:] + row_bits[:1])
    widths = (lead_width, trail_width)
    offsets = jnp.stack([row_index * lead_width, col_index * trail_width]).astype(jnp.int32)
    [weights] = fetched(
        functools.partial(fetch_weights, widths),
        (offsets,),
        (),
        [(2, 2 * sum(widths), 2 * C)],
        np.stack(split_table(channel_table())),
    )
    own = record.reshape(2, samples // LANES, LANES).transpose(1, 0, 2)
    own = own.reshape(1, 2 * samples // LANES, LANES)
    dft = np.stack([np.stack(split_table(window_table(odd))) for odd in range(2)])
    blocks, dft = fetched(fetch_whole, (), (own,), [own.shape, dft.shape], dft)
    for stage, bit in enumerate(order):
        route = [(i, i ^ (1 << bit)) for i in range(devices)]
        received = lax.ppermute(blocks if stage else own, axes, route)
        blocks = jnp.concatenate([blocks, received], axis=0)
        if stage == 0:
            blocks, dft = lax.optimization_barrier((blocks, dft))
        if stage == 1:
            blocks, weights = lax.optimization_barrier((blocks, weights))

    key = slot_of(me, order).astype(jnp.int32).reshape(1)
    height = trail_width * windows
    pattern = max(8, windows)
    sizes = (devices, widths, windows)
    vmem = pl.BlockSpec(memory_space=pltpu.VMEM)
    smem = pl.BlockSpec(memory_space=pltpu.SMEM)
    out = pl.pallas_call(
        functools.partial(kernel, order, sizes),
        out_shape=jax.ShapeDtypeStruct((lead_width * height * 4, LANES), jnp.float32),
        in_specs=[smem, vmem, vmem, vmem],
        out_specs=pl.BlockSpec(memory_space=pltpu.HBM),
        scratch_shapes=[
            pltpu.VMEM((2, 2, 2, devices * samples // LANES + SUBLANES, LANES), jnp.float32),
            pltpu.VMEM((4, lead_width * pattern, LANES), jnp.float32),
            pltpu.VMEM((4, height, LANES), jnp.float32),
            pltpu.VMEM((2, 2, GROUP * height, 2 * LANES), jnp.float32),
            pltpu.VMEM((2, 2, GROUP * height, 2 * LANES), jnp.float32),
            pltpu.VMEM((lead_width * height * 4, LANES), jnp.float32),
            pltpu.SemaphoreType.DMA((lead_width // GROUP,)),
        ],
        compiler_params=pltpu.CompilerParams(vmem_limit_bytes=40 * 2**20),
        cost_estimate=pl.CostEstimate(flops=10**10, bytes_accessed=10**7, transcendentals=0),
    )(key, blocks, weights, dft)
    out = out.reshape(lead_width, trail_width, windows, 2, 2, LANES)
    return out.transpose(0, 1, 2, 4, 3, 5).reshape(
        lead_width, trail_width, windows, 2, P_SIZE
    )


def solution(mesh):
    return jax.shard_map(
        local,
        mesh=mesh,
        in_specs=(P(None, ("row", "col")),),
        out_specs=P("row", "col", None, None, None),
        check_vma=False,
    )
```
